8 devices in a mesh: dp: 2 (over z, y), tp: 4 (over x, core).
Axes of the slice: x: 2, y: 2, z: 1, core: 2. Of those that a mesh axis runs over, the one named last changes fastest.
Arguments:
- x: bfloat16 [2, 2048, 2560], P('dp', 'tp')
- dy: bfloat16 [2, 2048, 2560], P('dp', 'tp')
- wq: bfloat16 [2560, 4096], P('dp', 'tp')
- wk: bfloat16 [2560, 1024], P('dp', 'tp')
- wv: bfloat16 [2560, 1024], P('dp', 'tp')
- wo: bfloat16 [4096, 2560], P(('tp', 'dp'))
- w_gate: bfloat16 [2560, 9728], P('dp', 'tp')
- w_up: bfloat16 [2560, 9728], P('dp', 'tp')
- w_down: bfloat16 [9728, 2560], P(('tp', 'dp'))
Outputs:
- output 1: bfloat16 [2, 2048, 2560], P('dp', 'tp')
- output 2: bfloat16 [2560, 4096], P('dp', 'tp')
- output 3: bfloat16 [2560, 1024], P('dp', 'tp')
- output 4: bfloat16 [2560, 1024], P('dp', 'tp')
- output 5: bfloat16 [4096, 2560], P(('tp', 'dp'))
- output 6: bfloat16 [2560, 9728], P('dp', 'tp')
- output 7: bfloat16 [2560, 9728], P('dp', 'tp')
- output 8: bfloat16 [9728, 2560], P(('tp', 'dp'))
All inputs are finite; a program needn't handle non-finite values.
Results may differ from the reference program's by a relative error of at most 0.024.
Values are sent between devices in bfloat16 or wider.
A program may use at most 2 GiB of HBM per device.

```python
import jax
import jax.numpy as jnp
from jax import lax

SEQUENCES = 2
TOKENS = 2048
D = 2560
HEADS = 32
KV_HEADS = 8
HEAD = 128
FF = 9728
THETA = 10000
NAMES = ("wq", "wk", "wv", "wo", "w_gate", "w_up", "w_down")
SHAPES = {
    "wq": (D, HEADS * HEAD),
    "wk": (D, KV_HEADS * HEAD),
    "wv": (D, KV_HEADS * HEAD),
    "wo": (HEADS * HEAD, D),
    "w_gate": (D, FF),
    "w_up": (D, FF),
    "w_down": (FF, D),
}


def bump(key, n, height):
    away = (jnp.arange(n, dtype=jnp.int32) - jax.random.randint(key, (), 0, n, jnp.int32)) % n
    return jnp.where(away < n // 8, height, 1.0)


def together(key, own, strength):
    shared = jax.random.normal(key, own.shape[1:], jnp.float32)
    return (own + strength * shared) * lax.rsqrt(1 + strength * strength)


def setup_inputs(seed: int = 0, part: int = 0) -> dict:
    kx, kdy, ka, kb, kz, kf, kh, kl, *kw = jax.random.split(jax.random.key(seed), 8 + len(NAMES))
    shape = (SEQUENCES, TOKENS, D)
    much_x, much_dy = jax.random.uniform(kz, (2,), jnp.float32, 0.0, 1.0)
    loud = 2.0 ** jax.random.uniform(jax.random.fold_in(kz, 1), (), jnp.float32, -1.0, 2.0)
    halves = 2.0 ** jax.random.uniform(kl, (2,), jnp.float32, -1.0, 1.0)
    times = {"wq": 1.0, "wk": 1.0, "wv": 2.0, "wo": halves[0], "w_gate": 1.0, "w_up": bump(kh, FF, 4.0), "w_down": halves[1]}
    x = together(ka, jax.random.normal(kx, shape, jnp.float32), much_x) * bump(kf, D, 4.0)
    dy = together(kb, jax.random.normal(kdy, shape, jnp.float32), much_dy)
    drawn = {"x": x.astype(jnp.bfloat16), "dy": (loud * dy * (SEQUENCES * TOKENS) ** -0.5).astype(jnp.bfloat16)}
    for key, name in zip(kw, NAMES, strict=True):
        drawn[name] = (jax.random.normal(key, SHAPES[name], jnp.float32) * SHAPES[name][0] ** -0.5 * times[name]).astype(jnp.bfloat16)
    return drawn


def matmul(a, w):
    return jnp.dot(a, w, preferred_element_type=jnp.float32).astype(jnp.bfloat16)


def normed(h):
    wide = h.astype(jnp.float32)
    scale = lax.rsqrt(jnp.mean(wide**2, -1, keepdims=True) + 1e-6)
    return (wide * scale).astype(jnp.bfloat16)


def turned(t, theta):
    half = t.shape[-1] // 2
    angle = jnp.arange(t.shape[0], dtype=jnp.float32)[:, None] * theta ** (-jnp.arange(half, dtype=jnp.float32) / half)
    cos, sin = jnp.cos(angle)[:, None], jnp.sin(angle)[:, None]
    a, b = t[..., :half].astype(jnp.float32), t[..., half:].astype(jnp.float32)
    return jnp.concatenate([a * cos - b * sin, b * cos + a * sin], -1).astype(jnp.bfloat16)


def seen_by(q, k, v):
    tokens, kv = q.shape[0], k.shape[1]
    q = q.reshape(tokens, kv, -1, q.shape[-1])
    scores = jnp.einsum("tgsd,ugd->gstu", q.astype(jnp.float32), k.astype(jnp.float32)) * q.shape[-1] ** -0.5
    place = jnp.arange(tokens)
    weights = jax.nn.softmax(jnp.where(place[:, None] >= place, scores, -jnp.inf), -1).astype(jnp.bfloat16)
    return jnp.einsum("gstu,ugd->tgsd", weights.astype(jnp.float32), v.astype(jnp.float32)).astype(jnp.bfloat16).reshape(tokens, -1)


def layer(h, w):
    a = normed(h)
    q, k = (turned(matmul(a, w[name]).reshape(h.shape[0], -1, HEAD), THETA) for name in ("wq", "wk"))
    h = h + matmul(seen_by(q, k, matmul(a, w["wv"]).reshape(h.shape[0], -1, HEAD)), w["wo"])
    b = normed(h)
    gate = jnp.dot(b, w["w_gate"], preferred_element_type=jnp.float32)
    up = jnp.dot(b, w["w_up"], preferred_element_type=jnp.float32)
    return h + matmul((jax.nn.silu(gate) * up).astype(jnp.bfloat16), w["w_down"])


def reference(x, dy, wq, wk, wv, wo, w_gate, w_up, w_down):
    weights = dict(zip(NAMES, (wq, wk, wv, wo, w_gate, w_up, w_down), strict=True))

    def take(so_far, sequence):
        h, by_y = sequence
        _, back = jax.vjp(lambda w, h: layer(h, w), weights, h)
        by_weights, by_h = back(by_y)
        return jax.tree.map(lambda total, term: total + term.astype(jnp.float32), so_far, by_weights), by_h

    none_yet = {name: jnp.zeros(w.shape, jnp.float32) for name, w in weights.items()}
    by_weights, by_x = lax.scan(take, none_yet, (x, dy))
    return (by_x, *(by_weights[name].astype(jnp.bfloat16) for name in NAMES))
```

```python
import functools

import jax
import jax.numpy as jnp
from jax import lax
from jax.experimental import pallas as pl
from jax.experimental.pallas import tpu as pltpu
from jax.sharding import PartitionSpec as P

NEG = -1e30
HIDDEN = 2 * NEG
LOG2E = 1.4426950408889634
HEAD = 128
THETA = 10000
Q, KV, G = 8, 2, 4
BLK = 512
TOK = 2048
D = 2560
HD = D // 2
SCALE = HEAD**-0.5
VMEM = 60 * 2**20
F32, BF = jnp.float32, jnp.bfloat16


def _dot(a, b, ca, cb):
    return lax.dot_general(a, b, (((ca,), (cb,)), ((), ())), preferred_element_type=F32)


def _turn(x, cos, sin):
    return x * cos + pltpu.roll(x, HEAD // 2, 1) * sin


def _gap():
    return lax.broadcasted_iota(jnp.int32, (BLK, BLK), 1) - lax.broadcasted_iota(jnp.int32, (BLK, BLK), 0)


def _lanes(n, width=HEAD):
    return slice(n * width, (n + 1) * width)


def _attn_fwd(s_ref, q_ref, k_ref, v_ref, cos_ref, sin_ref, o_ref, lse_ref, qr_ref, kr_ref, top_s, mix_s):
    iq, t, d = pl.program_id(0), s_ref[0], s_ref[1]
    e = SCALE * LOG2E

    @pl.when(iq == 0)
    def _():
        for p in range(TOK // BLK):
            rows = _lanes(p, BLK)
            for n in range(KV):
                kr_ref[rows, _lanes(n)] = _turn(k_ref[rows, _lanes(n)].astype(F32), cos_ref[rows, :], sin_ref[rows, :]).astype(BF)

    mine = pl.ds(pl.multiple_of((iq ^ t) * BLK, BLK), BLK)
    cos, sin = cos_ref[mine, :], sin_ref[mine, :]
    for h in range(Q):
        qr_ref[:, _lanes(h)] = _turn(q_ref[:, _lanes(h)].astype(F32), cos, sin).astype(BF)
    top_s[...] = jnp.full_like(top_s, NEG)
    mix_s[...] = jnp.zeros_like(mix_s)
    ones = jnp.ones((8, BLK), BF)

    def block(j, masked):
        here = pl.ds(pl.multiple_of((j ^ t) * BLK, BLK), BLK)
        scores = [_dot(kr_ref[here, _lanes(h // G)], qr_ref[:, _lanes(h)], 1, 1) for h in range(Q)]
        ok = _gap() >= 0 if masked else None
        weights, keeps = [], []
        for h, s in enumerate(scores):
            if masked:
                s = jnp.where(ok, s, HIDDEN)
            old = top_s[h : h + 1, :]
            top = jnp.maximum(old, s.max(axis=0, keepdims=True))
            top_s[h : h + 1, :] = top
            weights.append(jnp.exp2((s - top) * e).astype(BF))
            keeps.append(jnp.exp2((old - top) * e))
        for h in range(Q):
            values = jnp.concatenate([v_ref[here, _lanes(h // G)].T, ones], axis=0)
            mix_s[h] = mix_s[h] * keeps[h] + _dot(values, weights[h], 1, 0)

    lax.fori_loop(0, iq, lambda j, _: block(j, False), None)
    block(iq, True)
    for h in range(Q):
        total = mix_s[h, HEAD : HEAD + 1, :]
        at = pl.multiple_of(((h // G) ^ d) * G * HEAD + (h % G) * HEAD, HEAD)
        o_ref[:, pl.ds(at, HEAD)] = (mix_s[h, :HEAD, :] * (1 / total)).T.astype(BF)
        lse_ref[h // G, h % G : h % G + 1, :] = top_s[h : h + 1, :] * SCALE + jnp.log(total)


def attn_fwd(place, qkv, cos, sin):
    whole = lambda iq, s: (0, 0)
    rows = lambda iq, s: (iq ^ s[0], 0)
    table = pl.BlockSpec((TOK, HEAD), whole)
    return pl.pallas_call(
        _attn_fwd,
        grid_spec=pltpu.PrefetchScalarGridSpec(
            num_scalar_prefetch=1,
            grid=(TOK // BLK,),
            in_specs=[pl.BlockSpec((BLK, Q * HEAD), rows), pl.BlockSpec((TOK, KV * HEAD), lambda iq, s: (0, 4)),
                      pl.BlockSpec((TOK, KV * HEAD), lambda iq, s: (0, 5)), table, table],
            out_specs=[pl.BlockSpec((BLK, Q * HEAD), rows), pl.BlockSpec((KV, G, BLK), lambda iq, s: (0, 0, iq ^ s[0])),
                       pl.BlockSpec((BLK, Q * HEAD), rows), pl.BlockSpec((TOK, KV * HEAD), whole)],
            scratch_shapes=[pltpu.VMEM((Q, BLK), F32), pltpu.VMEM((Q, HEAD + 8, BLK), F32)],
        ),
        out_shape=[jax.ShapeDtypeStruct((TOK, Q * HEAD), BF), jax.ShapeDtypeStruct((KV, G, TOK), F32),
                   jax.ShapeDtypeStruct((TOK, Q * HEAD), BF), jax.ShapeDtypeStruct((TOK, KV * HEAD), BF)],
        compiler_params=pltpu.CompilerParams(dimension_semantics=("arbitrary",), vmem_limit_bytes=VMEM),
        cost_estimate=pl.CostEstimate(flops=30 * 10**9, transcendentals=Q * TOK * TOK // 2, bytes_accessed=16 * 2**20),
        name="attn_fwd",
    )(place, qkv, qkv, qkv, cos, sin)


def _attn_bwd(s_ref, q_ref, k_ref, v_ref, do_ref, o_ref, lse_ref, cos_ref, sin_ref, out_ref, dq_s, dk_s, dv_s):
    kv, iq, t = pl.program_id(0), pl.program_id(1), s_ref[0]
    e = SCALE * LOG2E
    mine = pl.ds(pl.multiple_of((iq ^ t) * BLK, BLK), BLK)

    @pl.when(iq == 0)
    def _():
        dk_s[...] = jnp.zeros_like(dk_s)
        dv_s[...] = jnp.zeros_like(dv_s)

    dq_s[...] = jnp.zeros_like(dq_s)
    lses = [lse_ref[0, h : h + 1, :] * LOG2E for h in range(G)]
    deltas = []
    for h in range(G):
        both = do_ref[:, _lanes(h)].astype(F32) * o_ref[:, _lanes(h)].astype(F32)
        deltas.append(both.T.sum(axis=0, keepdims=True))

    def block(j, masked):
        here = pl.ds(pl.multiple_of((j ^ t) * BLK, BLK), BLK)
        qs = [q_ref[:, _lanes(h)] for h in range(G)]
        dos = [do_ref[:, _lanes(h)] for h in range(G)]
        scores = [_dot(k_ref[here, :], x, 1, 1) for x in qs]
        dps = [_dot(v_ref[here, :], x, 1, 1) for x in dos]
        ok = _gap() >= 0 if masked else None
        for h in range(G):
            p = jnp.exp2(scores[h] * e - lses[h])
            if masked:
                p = jnp.where(ok, p, 0.0)
            ds = (p * (dps[h] - deltas[h])).astype(BF)
            dv_s[here, :] += _dot(p.astype(BF), dos[h], 1, 0)
            dk_s[here, :] += _dot(ds, qs[h], 1, 0)
            dq_s[:, _lanes(h, BLK)] += _dot(k_ref[here, :].T, ds, 1, 0)

    lax.fori_loop(0, iq, lambda j, _: block(j, False), None)
    block(iq, True)

    def back(x, cos, sin):
        x = x.astype(BF).astype(F32)
        return (x * cos - pltpu.roll(x, HEAD // 2, 1) * sin).astype(BF)

    for h in range(G):
        at = pl.multiple_of(kv * G * HEAD + h * HEAD, HEAD)
        out_ref[mine, pl.ds(at, HEAD)] = back((dq_s[:, _lanes(h, BLK)] * SCALE).T, cos_ref[mine, :], sin_ref[mine, :])

    @pl.when(iq == pl.num_programs(1) - 1)
    def _():
        out_ref[:, pl.ds(pl.multiple_of(Q * HEAD + kv * HEAD, HEAD), HEAD)] = back(dk_s[...] * SCALE, cos_ref[...], sin_ref[...])
        out_ref[:, pl.ds(pl.multiple_of((Q + KV) * HEAD + kv * HEAD, HEAD), HEAD)] = dv_s[...].astype(BF)


def attn_bwd(place, qr, kr, qkv, d_heads, heads, lse, cos, sin):
    rows = lambda kv, iq, s: (iq ^ s[0], kv)
    rot = lambda kv, iq, s: (iq ^ s[0], kv ^ s[1])
    whole = lambda kv, iq, s: (0, 0)
    one = pl.Buffered(1)
    table = pl.BlockSpec((TOK, HEAD), whole, pipeline_mode=one)
    wide = pl.BlockSpec((BLK, G * HEAD), rows)
    wide_rot = pl.BlockSpec((BLK, G * HEAD), rot)
    return pl.pallas_call(
        _attn_bwd,
        grid_spec=pltpu.PrefetchScalarGridSpec(
            num_scalar_prefetch=1,
            grid=(KV, TOK // BLK),
            in_specs=[wide, pl.BlockSpec((TOK, HEAD), lambda kv, iq, s: (0, kv)), pl.BlockSpec((TOK, HEAD), lambda kv, iq, s: (0, 10 + kv)),
                      wide_rot, wide_rot, pl.BlockSpec((1, G, BLK), lambda kv, iq, s: (kv, 0, iq ^ s[0])), table, table],
            out_specs=pl.BlockSpec((TOK, (Q + 2 * KV) * HEAD), whole),
            scratch_shapes=[pltpu.VMEM((HEAD, G * BLK), F32), pltpu.VMEM((TOK, HEAD), F32), pltpu.VMEM((TOK, HEAD), F32)],
        ),
        out_shape=jax.ShapeDtypeStruct((TOK, (Q + 2 * KV) * HEAD), BF),
        compiler_params=pltpu.CompilerParams(dimension_semantics=("arbitrary", "arbitrary"), vmem_limit_bytes=VMEM),
        cost_estimate=pl.CostEstimate(flops=55 * 10**9, transcendentals=Q * TOK * TOK // 2, bytes_accessed=24 * 2**20),
        name="attn_bwd",
    )(place, qr, kr, qkv, d_heads, heads, lse, cos, sin)


def _mlp(b_ref, dy_ref, g0, g1, u0, u1, wd, hid_ref, dg_ref, du_ref, db_ref):
    b0, b1 = b_ref[:, :HD], b_ref[:, HD:]
    gate = _dot(b0, g0[...], 1, 0) + _dot(b1, g1[...], 1, 0)
    up = _dot(b0, u0[...], 1, 0) + _dot(b1, u1[...], 1, 0)
    dh = _dot(dy_ref[...], wd[...], 1, 1).astype(BF).astype(F32)
    sig = jax.nn.sigmoid(gate)
    silu = gate * sig
    hid_ref[...] = (silu * up).astype(BF)
    dg = (dh * up * (sig * (1 + gate * (1 - sig)))).astype(BF)
    du = (dh * silu).astype(BF)
    dg_ref[...], du_ref[...] = dg, du
    db_ref[:, :HD] = (_dot(dg, g0[...], 1, 1) + _dot(du, u0[...], 1, 1)).astype(BF)
    db_ref[:, HD:] = (_dot(dg, g1[...], 1, 1) + _dot(du, u1[...], 1, 1)).astype(BF)


def mlp(b, dy, g0, g1, u0, u1, wd, tile=256):
    n, ff = b.shape[0], wd.shape[0]
    tok = lambda width: pl.BlockSpec((tile, width), lambda i: (i, 0))
    held = lambda w: pl.BlockSpec(w.shape, lambda i: (0, 0), pipeline_mode=pl.Buffered(1))
    shape = lambda width: jax.ShapeDtypeStruct((n, width), BF)
    return pl.pallas_call(
        _mlp,
        grid=(n // tile,),
        in_specs=[tok(D), tok(D), *(held(w) for w in (g0, g1, u0, u1, wd))],
        out_specs=[tok(ff), tok(ff), tok(ff), tok(D)],
        out_shape=[shape(ff), shape(ff), shape(ff), shape(D)],
        compiler_params=pltpu.CompilerParams(dimension_semantics=("arbitrary",), vmem_limit_bytes=VMEM),
        cost_estimate=pl.CostEstimate(flops=10 * n * ff * D, transcendentals=n * ff, bytes_accessed=2 * (3 * n * ff + 3 * n * D + 3 * D * ff)),
        name="mlp",
    )(b, dy, g0, g1, u0, u1, wd)


def normed(h):
    wide = h.astype(F32)
    scale = lax.rsqrt(jnp.mean(wide**2, -1, keepdims=True) + 1e-6)
    return (wide * scale).astype(BF)


def to_y(v):
    return lax.ppermute(v, "dp", [(0, 1), (1, 0)])


def to_x(v):
    return lax.ppermute(v, "tp", [(i, i ^ 2) for i in range(4)])


def to_core(v):
    return lax.ppermute(v, "tp", [(i, i ^ 1) for i in range(4)])


def add(*terms):
    return sum(v.astype(F32) for v in terms).astype(BF)


def after(v, *others):
    return lax.optimization_barrier((v, *others))[0]


def gather4(own, from_x=None):
    x = to_x(own)
    return jnp.concatenate([own, to_core(own), x, to_core(x)], axis=0)


def blocks(v):
    return [v[i : i + BLK] for i in range(0, v.shape[0], BLK)]


def scatter4(v):
    v0, v1, v2, v3 = blocks(v)
    s2 = add(v2, to_core(v3))
    return add(v0, to_core(v1), to_x(s2))


def dot_t(a, b):
    return _dot(a, b, 0, 0).astype(BF)


def solution(mesh):
    def step(x, dy, wq, wk, wv, wo, wg, wu, wd):
        d, t = lax.axis_index("dp"), lax.axis_index("tp")
        place = jnp.stack([t, d]).astype(jnp.int32)
        x, dy = x[0], dy[0]
        ff = wd.shape[0]
        rot = lambda v, k: jnp.where(k == 0, v, jnp.concatenate([v[:, HD:], v[:, :HD]], axis=1))
        pick = lambda k, w: jnp.where(k == 0, w[:, :ff], w[:, ff:])
        join = lambda mine, other: jnp.where(d == 0, jnp.concatenate([mine, other], 1), jnp.concatenate([other, mine], 1))

        w_own = jnp.concatenate([wq, wk, wv], axis=1)
        w_rot = jnp.concatenate([w_own, to_y(w_own)], axis=0)
        a = gather4(rot(normed(x), d))
        wo_rot = jnp.concatenate([wo, to_y(wo)], axis=0)
        place_of = ((jnp.arange(4) ^ t) * BLK)[:, None] + jnp.arange(BLK)
        half = HEAD // 2
        angle = place_of.reshape(TOK, 1).astype(F32) * THETA ** (-jnp.arange(half, dtype=F32) / half)
        cos, sin = jnp.cos(angle), jnp.sin(angle)
        cos, sin = jnp.concatenate([cos, cos], 1), jnp.concatenate([-sin, sin], 1)
        qkv = _dot(a, w_rot, 1, 0).astype(BF)
        heads, lse, qr, kr = attn_fwd(place, qkv, cos, sin)
        out = scatter4(_dot(heads, wo_rot, 1, 0).astype(BF))
        h = add(x, out)

        g0, u0 = pick(d, wg), pick(d, wu)
        g1 = to_y(pick(1 - d, wg))
        b, norm_back = jax.vjp(normed, h)
        b_own = gather4(rot(b, d))
        b_oth = gather4(to_y(rot(b, 1 - d)))
        u1 = to_y(after(pick(1 - d, wu), b))
        dy_own = gather4(dy)
        dy_oth = gather4(to_y(after(dy, b)))
        hid_t, dg_t, du_t, db_t = mlp(b_oth, dy_oth, g0, g1, u0, u1, wd)
        hid_o, dg_o, du_o, db_o = mlp(b_own, dy_own, g0, g1, u0, u1, wd)
        v4, v5, v6, v7 = blocks(db_t)
        s6 = add(v6, to_core(v7))
        s4 = add(v4, to_core(v5), to_x(s6))
        v0, v1, v2, v3 = blocks(db_o)
        s2 = add(v2, to_core(v3))
        db = add(rot(add(v0, to_core(v1), to_x(s2)), d), rot(to_y(s4), 1 - d))
        dh = add(dy, norm_back(db)[0])
        two = lambda m, n: jnp.concatenate([m, n], axis=0)
        b_all, dg, du = two(b_own, b_oth), two(dg_o, dg_t), two(du_o, du_t)
        g_wg = join(dot_t(b_all[:, :HD], dg), to_y(dot_t(b_all[:, HD:], dg)))
        g_wu = join(dot_t(b_all[:, :HD], du), to_y(dot_t(b_all[:, HD:], du)))
        g_wd = dot_t(two(hid_o, hid_t), two(dy_own, dy_oth))

        dh_all = gather4(dh)
        d_heads = _dot(dh_all, wo_rot, 1, 1).astype(BF)
        half_rows = heads.shape[1] // 2
        g_wo = add(dot_t(heads[:, :half_rows], dh_all), to_y(dot_t(heads[:, half_rows:], dh_all)))
        dqkv = attn_bwd(place, qr, kr, qkv, d_heads, heads, lse, cos, sin)
        g_w = add(dot_t(a[:, :HD], dqkv), to_y(dot_t(a[:, HD:], dqkv)))
        da = rot(scatter4(_dot(dqkv, w_rot, 1, 1).astype(BF)), d)
        dx = add(dh, jax.vjp(normed, x)[1](da)[0])
        nq, nk = wq.shape[1], wk.shape[1]
        return dx[None], g_w[:, :nq], g_w[:, nq : nq + nk], g_w[:, nq + nk :], g_wo, g_wg, g_wu, g_wd

    states, by_columns, by_rows = P("dp", "tp", None), P("dp", "tp"), P(("tp", "dp"), None)
    weights = (by_columns, by_columns, by_columns, by_rows, by_columns, by_columns, by_rows)
    return jax.shard_map(step, mesh=mesh, in_specs=(states, states, *weights), out_specs=(states, *weights), check_vma=False)
```
